16 devices in a mesh: dp: 2 (over z), tp: 8 (over y, x, core).
Axes of the slice: x: 2, y: 2, z: 2, core: 2. Of those that a mesh axis runs over, the one named last changes fastest.
Arguments:
- x: bfloat16 [512, 1024], P('dp'), parts along dimension 0
- cache_len: int32 [512], P('dp'), parts along dimension 0
- k_cache: bfloat16 [2, 512, 16, 128, 64], P(None, 'dp', 'tp'), parts along dimension 1
- v_cache: bfloat16 [2, 512, 16, 128, 64], P(None, 'dp', 'tp'), parts along dimension 1
- norm_gain: float32 [2, 2, 1024], replicated
- norm_bias: float32 [2, 2, 1024], replicated
- w_qkv: bfloat16 [2, 1024, 3, 16, 64], P(None, None, None, 'tp')
- b_qkv: bfloat16 [2, 3, 16, 64], P(None, None, 'tp')
- w_out: bfloat16 [2, 16, 64, 1024], P(None, 'tp')
- b_out: bfloat16 [2, 1024], replicated
- w_up: bfloat16 [2, 1024, 4096], P(None, None, 'tp')
- b_up: bfloat16 [2, 4096], P(None, 'tp')
- w_down: bfloat16 [2, 4096, 1024], P(None, 'tp')
- b_down: bfloat16 [2, 1024], replicated
Outputs:
- output 1: bfloat16 [512, 1024], P('dp'), parts along dimension 0
- output 2: bfloat16 [2, 512, 16, 128, 64], P(None, 'dp', 'tp'), parts along dimension 1
- output 3: bfloat16 [2, 512, 16, 128, 64], P(None, 'dp', 'tp'), parts along dimension 1
There are 2 independent parts. The reference program is written for one: setup_inputs(seed, part) draws one part's arguments, and reference() takes and returns one part's arrays. A program takes and returns all parts, laid end to end along the dimension named above; an argument that names none is the same for every part.
All inputs are finite; a program needn't handle non-finite values.
Results may differ from the reference program's by a relative error of at most 0.0166085.
Values are sent between devices in bfloat16 or wider.
A program may use at most 1 GiB of HBM per device.

```python
import jax
import jax.numpy as jnp
from jax import lax

D = 1024
HEADS = 16
HEAD = 64
BATCH = 256
SMAX = 128
LAYERS = 2
FFN = 4096
NORM_EPS = 1e-5


def setup_inputs(seed: int = 0, part: int = 0) -> dict:
    part_keys = jax.random.split(jax.random.fold_in(jax.random.key(seed), part), 5)
    shared_keys = jax.random.split(jax.random.key(seed + 1), 10)
    x = jax.random.normal(part_keys[0], (BATCH, D), jnp.float32)
    raw_len = jax.random.randint(part_keys[1], (BATCH,), 0, SMAX)
    full_row = jax.random.randint(part_keys[2], (), 0, BATCH)
    cache_len = jnp.where(jnp.arange(BATCH) == full_row, SMAX - 1, raw_len).astype(jnp.int32)
    cache_shape = (LAYERS, BATCH, HEADS, SMAX, HEAD)
    k_cache = 1.5 * jax.random.normal(part_keys[3], cache_shape, jnp.float32)
    v_cache = jax.random.normal(part_keys[4], cache_shape, jnp.float32)
    norm_gain = 1.0 + 0.3 * jax.random.normal(shared_keys[0], (LAYERS, 2, D), jnp.float32)
    norm_bias = 0.3 * jax.random.normal(shared_keys[1], (LAYERS, 2, D), jnp.float32)
    w_qkv = jax.random.normal(shared_keys[2], (LAYERS, D, 3, HEADS, HEAD), jnp.float32) * D ** -0.5
    b_qkv = 0.5 * jax.random.normal(shared_keys[3], (LAYERS, 3, HEADS, HEAD), jnp.float32)
    w_out = jax.random.normal(shared_keys[4], (LAYERS, HEADS, HEAD, D), jnp.float32) * (HEADS * HEAD) ** -0.5
    b_out = 0.3 * jax.random.normal(shared_keys[5], (LAYERS, D), jnp.float32)
    w_up = jax.random.normal(shared_keys[6], (LAYERS, D, FFN), jnp.float32) * D ** -0.5
    b_up = 0.5 * jax.random.normal(shared_keys[7], (LAYERS, FFN), jnp.float32)
    w_down = jax.random.normal(shared_keys[8], (LAYERS, FFN, D), jnp.float32) * FFN ** -0.5
    b_down = 0.3 * jax.random.normal(shared_keys[9], (LAYERS, D), jnp.float32)
    return {
        'x': x.astype(jnp.bfloat16),
        'cache_len': cache_len,
        'k_cache': k_cache.astype(jnp.bfloat16),
        'v_cache': v_cache.astype(jnp.bfloat16),
        'norm_gain': norm_gain,
        'norm_bias': norm_bias,
        'w_qkv': w_qkv.astype(jnp.bfloat16),
        'b_qkv': b_qkv.astype(jnp.bfloat16),
        'w_out': w_out.astype(jnp.bfloat16),
        'b_out': b_out.astype(jnp.bfloat16),
        'w_up': w_up.astype(jnp.bfloat16),
        'b_up': b_up.astype(jnp.bfloat16),
        'w_down': w_down.astype(jnp.bfloat16),
        'b_down': b_down.astype(jnp.bfloat16),
    }


def layer_norm(vec, gain_vec, bias_vec):
    vec_f = vec.astype(jnp.float32)
    row_mean = jnp.mean(vec_f, axis=-1, keepdims=True)
    centered = vec_f - row_mean
    row_var = jnp.mean(centered * centered, axis=-1, keepdims=True)
    return (centered * lax.rsqrt(row_var + NORM_EPS) * gain_vec + bias_vec).astype(jnp.bfloat16)


def row_attention(row_args):
    q_row, k_row, v_row, kc_row, vc_row, len_row = row_args
    kc_new = lax.dynamic_update_slice_in_dim(kc_row, k_row[:, None, :], len_row, axis=1)
    vc_new = lax.dynamic_update_slice_in_dim(vc_row, v_row[:, None, :], len_row, axis=1)
    scores = jnp.einsum('hd,hjd->hj', q_row.astype(jnp.float32), kc_new.astype(jnp.float32)) * (HEAD ** -0.5)
    visible = jnp.arange(SMAX)[None, :] <= len_row
    scores = jnp.where(visible, scores, -1e30)
    attn_prob = jax.nn.softmax(scores, axis=-1).astype(jnp.bfloat16)
    attended = jnp.einsum('hj,hjd->hd', attn_prob.astype(jnp.float32), vc_new.astype(jnp.float32)).astype(jnp.bfloat16)
    return attended, kc_new, vc_new


def decoder_layer(x, cache_len, layer_par):
    gain_pair, bias_pair, w_qkv, b_qkv, w_out, b_out, w_up, b_up, w_down, b_down, kc_layer, vc_layer = layer_par
    hidden = layer_norm(x, gain_pair[0], bias_pair[0])
    qkv_flat = jnp.dot(hidden, w_qkv.reshape(D, 3 * HEADS * HEAD), preferred_element_type=jnp.float32)
    qkv_all = (qkv_flat.reshape(BATCH, 3, HEADS, HEAD) + b_qkv.astype(jnp.float32)).astype(jnp.bfloat16)
    attended, kc_new, vc_new = lax.map(row_attention, (qkv_all[:, 0], qkv_all[:, 1], qkv_all[:, 2], kc_layer, vc_layer, cache_len))
    attn_sum = jnp.dot(attended.reshape(BATCH, HEADS * HEAD), w_out.reshape(HEADS * HEAD, D), preferred_element_type=jnp.float32)
    x_mid = (x.astype(jnp.float32) + attn_sum + b_out.astype(jnp.float32)).astype(jnp.bfloat16)
    hidden_mlp = layer_norm(x_mid, gain_pair[1], bias_pair[1])
    up_act = jnp.maximum(jnp.dot(hidden_mlp, w_up, preferred_element_type=jnp.float32) + b_up.astype(jnp.float32), 0.0).astype(jnp.bfloat16)
    mlp_sum = jnp.dot(up_act, w_down, preferred_element_type=jnp.float32)
    x_new = (x_mid.astype(jnp.float32) + mlp_sum + b_down.astype(jnp.float32)).astype(jnp.bfloat16)
    return x_new, (kc_new, vc_new)


def reference(x, cache_len, k_cache, v_cache, norm_gain, norm_bias, w_qkv, b_qkv, w_out, b_out, w_up, b_up, w_down, b_down):
    def layer_step(carry, layer_par):
        return decoder_layer(carry, cache_len, layer_par)
    x_final, caches = lax.scan(layer_step, x, (norm_gain, norm_bias, w_qkv, b_qkv, w_out, b_out, w_up, b_up, w_down, b_down, k_cache, v_cache))
    return x_final, caches[0], caches[1]
```

```python
import functools

import jax
import jax.numpy as jnp
from jax import lax
from jax.experimental import pallas as pl
from jax.experimental.pallas import tpu as pltpu
from jax.sharding import PartitionSpec as P

F32 = jnp.float32
BF16 = jnp.bfloat16
EPS = 1e-5
MESH = pl.DeviceIdType.MESH
GB = 16


def norm_rows(xf, gain, bias):
    mean = jnp.mean(xf, axis=-1, keepdims=True)
    cen = xf - mean
    var = jnp.mean(cen * cen, axis=-1, keepdims=True)
    return (cen * lax.rsqrt(var + EPS) * gain + bias).astype(BF16)


def nt_dot(a, b):
    return lax.dot_general(a, b, (((1,), (1,)), ((), ())), preferred_element_type=F32)


def attn_kernel(layer, aliased, len_ref, gain_ref, bias_ref, bq_ref, x_hbm, w_hbm, k_hbm, v_hbm, *rest):
    if aliased:
        rest = rest[2:]
    k_out, v_out, a_ref, x_s, w_s, k_s, v_s, q_s, kvt_s, p_s, in_sem, out_sem, xw_sem = rest
    nb = x_s.shape[0]
    hd = 128
    smax = 128
    groups = nb // GB

    def rows(g):
        return pl.ds(pl.multiple_of(g * GB, GB), GB)

    def load(g):
        return [pltpu.make_async_copy(hbm.at[layer, rows(g)], buf.at[rows(g)], in_sem.at[t, g])
                for t, (hbm, buf) in enumerate(((k_hbm, k_s), (v_hbm, v_s)))]

    def save(g):
        return [pltpu.make_async_copy(buf.at[rows(g)], hbm.at[layer, rows(g)], out_sem.at[t, g])
                for t, (hbm, buf) in enumerate(((k_out, k_s), (v_out, v_s)))]

    cx = pltpu.make_async_copy(x_hbm, x_s, xw_sem.at[0])
    cw = pltpu.make_async_copy(w_hbm.at[layer], w_s, xw_sem.at[1])
    cx.start()
    cw.start()

    def start_loads(g, c):
        for cp in load(g):
            cp.start()
        return c

    cx.wait()
    cw.wait()
    lax.fori_loop(0, groups, start_loads, 0)
    if layer == 0:
        h = norm_rows(x_s[...].astype(F32), gain_ref[layer, 0:1, :], bias_ref[layer, 0:1, :])
    else:
        h = x_s[...]
    bq = bq_ref[layer].astype(F32)
    bq = jnp.concatenate([bq[t, j:j + 1] for t in range(3) for j in range(2)], axis=1)
    qkv = nt_dot(h, w_s[...]) + bq
    q_s[...] = qkv[:, :hd].astype(BF16)
    kvt = jnp.swapaxes(qkv[:, hd:], 0, 1).astype(BF16)
    for t in range(nb // 128):
        kvt_s[t] = kvt[:, t * 128:(t + 1) * 128]
    p_s[...] = jnp.zeros_like(p_s)

    row = lax.broadcasted_iota(jnp.int32, (GB, smax), 0)
    lane = lax.broadcasted_iota(jnp.int32, (GB, smax), 1)
    row_b = row.astype(F32).astype(BF16)
    lane_b = lane.astype(F32).astype(BF16)
    lane_h = lane // 64
    low_b = lane_b < 64
    zero = jnp.zeros((GB, hd), BF16)

    def weigh(g):
        o = nt_dot(p_s[...], v_s[rows(g)].reshape(GB * hd, smax))
        acc = jnp.zeros((GB, hd), F32)
        for i in range(GB):
            blk = o[:, i * hd:(i + 1) * hd]
            acc = jnp.where(row == i, jnp.where(lane_h == 0, blk[:GB], blk[GB:]), acc)
        a_ref[rows(g), :] = acc.astype(BF16)

    def group(g, carry):
        base = g * GB
        for cp in load(g):
            cp.wait()
        weigh(jnp.maximum(g - 1, 0))
        q16 = q_s[rows(g), :]
        lens = [len_ref[base + i] for i in range(GB)]
        lentile = jnp.zeros((GB, smax), jnp.int32)
        for i in range(GB):
            lentile = jnp.where(row == i, lens[i], lentile)
        tile = base // 128
        for i in range(GB):
            hit = lane_b == lens[i].astype(F32).astype(BF16)
            shift = lax.rem(lens[i] - (base + i) % 128 + 128, 128)
            for part, buf in ((0, k_s), (1, v_s)):
                cols = kvt_s[tile, part * hd:(part + 1) * hd, :]
                moved = pltpu.roll(cols, shift, 1)
                old = buf[base + i].reshape(hd // GB, GB, smax)
                buf[base + i] = jnp.where(hit[None], moved.reshape(hd // GB, GB, smax), old).reshape(2, 64, smax)
        for cp in save(g):
            cp.start()
        qh = [jnp.where(low_b, q16, zero), jnp.where(low_b, zero, q16)]
        qbd = jnp.concatenate(
            [jnp.concatenate([jnp.where(row_b == i, qh[h], zero) for i in range(GB)], axis=1) for h in range(2)], axis=0)
        s = jnp.dot(qbd, k_s[rows(g)].reshape(GB * hd, smax), preferred_element_type=F32) * 0.125
        seen = lane <= lentile
        s = jnp.where(jnp.concatenate([seen, seen], axis=0), s, -1e30)
        m = jnp.max(s, axis=-1, keepdims=True)
        ex = jnp.exp(s - m)
        p_s[...] = (ex / jnp.sum(ex, axis=-1, keepdims=True)).astype(BF16)
        return carry

    lax.fori_loop(0, groups, group, 0)
    weigh(groups - 1)

    def end_saves(g, c):
        for cp in save(g):
            cp.wait()
        return c

    lax.fori_loop(0, groups, end_saves, 0)


def attention(layer, cache_len, x, gain, bias, w_t, b_qkv, k_t, v_t, prev):
    nl, nb = k_t.shape[:2]
    vmem = pl.BlockSpec(memory_space=pltpu.VMEM)
    hbm = pl.BlockSpec(memory_space=pl.ANY)
    in_specs = [pl.BlockSpec(memory_space=pltpu.SMEM), vmem, vmem, vmem, hbm, hbm, hbm, hbm]
    operands = [cache_len, gain, bias, b_qkv, x, w_t, k_t, v_t]
    aliases = {}
    if prev is not None:
        in_specs += [hbm, hbm]
        operands += list(prev)
        aliases = {8: 0, 9: 1}
    groups = nb // GB
    return pl.pallas_call(
        functools.partial(attn_kernel, layer, prev is not None),
        in_specs=in_specs,
        out_specs=[hbm, hbm, vmem],
        out_shape=[jax.ShapeDtypeStruct(k_t.shape, BF16), jax.ShapeDtypeStruct(v_t.shape, BF16),
                   jax.ShapeDtypeStruct((nb, 128), BF16)],
        scratch_shapes=[
            pltpu.VMEM(x.shape, BF16), pltpu.VMEM(w_t.shape[1:], BF16),
            pltpu.VMEM(k_t.shape[1:], BF16), pltpu.VMEM(v_t.shape[1:], BF16),
            pltpu.VMEM((nb, 128), BF16), pltpu.VMEM((nb // 128, 256, 128), BF16), pltpu.VMEM((2 * GB, 128), BF16),
            pltpu.SemaphoreType.DMA((2, groups)), pltpu.SemaphoreType.DMA((2, groups)), pltpu.SemaphoreType.DMA((2,))],
        input_output_aliases=aliases,
        compiler_params=pltpu.CompilerParams(vmem_limit_bytes=63 * 2 ** 20),
        cost_estimate=pl.CostEstimate(flops=10 ** 9, bytes_accessed=2 ** 25, transcendentals=0),
        name=f"attention_{layer}",
    )(*operands)


def tail_kernel(layer, last, a_ref, x_in, gain_ref, bias_ref, bo_ref, bu_ref, bd_ref, wo_hbm, wu_hbm, wd_hbm, *rest):
    if last:
        out_ref, *rest = rest
        xrow_out = None
    else:
        out_ref, xrow_out, *rest = rest
    (wo, wu, wd, xs, hb, ob, act, own, dsend, drecv, csend, crecv, w_sem, x_sem,
     ds_sem, dr_sem, cs_sem, cr_sem, gs_sem, gr_sem) = rest
    nb, width = hb.shape
    me = lax.axis_index("tp")
    core = lax.rem(me, 2)
    chip = lax.div(me, 2)
    half = nb // 2
    cut = nb // 8
    far = (3, 1, 2)

    def chip_at(dist):
        xb, yb = lax.rem(chip, 2), lax.div(chip, 2)
        dx, dy = dist % 2, dist // 2
        nx = xb + dx - 2 * dx * xb
        ny = yb + dy - 2 * dy * yb
        return ny * 2 + nx

    sibling = chip * 2 + 1 - core
    peers = {d: chip_at(d) * 2 + core for d in far}

    loads = [pltpu.make_async_copy(h.at[layer], v, w_sem.at[i]) for i, (h, v) in enumerate(((wo_hbm, wo), (wu_hbm, wu), (wd_hbm, wd)))]
    for cp in loads:
        cp.start()
    row0 = pl.multiple_of((core * 4 + chip) * cut, cut)
    if layer == 0:
        cx = pltpu.make_async_copy(x_in.at[pl.ds(row0, cut)], xs, x_sem)
        cx.start()

    barrier = pltpu.get_barrier_semaphore()
    for dev in [sibling] + [peers[d] for d in far]:
        pl.semaphore_signal(barrier, inc=1, device_id={"tp": dev}, device_id_type=MESH)
    pl.semaphore_wait(barrier, 4)

    def block(ref, c, k):
        return ref.at[pl.ds(pl.multiple_of((k * 4 + c) * cut, cut), cut)]

    def scatter(r, act_ref, w_ref):
        other = pl.multiple_of((1 - core) * half, half)
        dsend[r] = jnp.dot(act_ref[pl.ds(other, half), :], w_ref[...], preferred_element_type=F32).astype(BF16)
        d2d = {}
        for n, d in enumerate(far + (0,)):
            cs = pl.ds(pl.multiple_of(chip_at(d) * cut, cut), cut)
            d2d[d] = pltpu.make_async_remote_copy(dsend.at[r, cs], drecv.at[r, cs], ds_sem.at[r, n], dr_sem.at[r, n],
                                                  device_id={"tp": sibling}, device_id_type=MESH)
            d2d[d].start()
        own[...] = jnp.dot(act_ref[pl.ds(pl.multiple_of(core * half, half), half), :], w_ref[...], preferred_element_type=F32)
        sends = []
        for n, d in enumerate(far):
            cs = pl.ds(pl.multiple_of(chip_at(d) * cut, cut), cut)
            d2d[d].wait_recv()
            csend[r, n] = (own[cs, :] + drecv[r, cs, :].astype(F32)).astype(BF16)
            cp = pltpu.make_async_remote_copy(csend.at[r, n], crecv.at[r, n], cs_sem.at[r, n], cr_sem.at[r, n],
                                              device_id={"tp": peers[d]}, device_id_type=MESH)
            cp.start()
            sends.append(cp)
        cs = pl.ds(pl.multiple_of(chip * cut, cut), cut)
        d2d[0].wait_recv()
        total = own[cs, :] + drecv[r, cs, :].astype(F32)
        for n in (1, 2, 0):
            sends[n].wait_recv()
            total = total + crecv[r, n].astype(F32)
        return total, [*d2d.values(), *sends]

    def gather(r, buf, rows):
        block(buf, chip, core)[...] = rows
        mine = block(buf, chip, core)
        first = {}
        for n, (d, dev) in enumerate([(d, peers[d]) for d in far] + [(0, sibling)]):
            first[d] = pltpu.make_async_remote_copy(mine, mine, gs_sem.at[r, n], gr_sem.at[r, n],
                                                    device_id={"tp": dev}, device_id_type=MESH)
            first[d].start()
        second = []
        for n, d in ((1, 1), (2, 2), (0, 3)):
            c = chip_at(d)
            pltpu.make_async_remote_copy(mine, block(buf, c, core), gs_sem.at[r, n], gr_sem.at[r, n],
                                         device_id={"tp": peers[d]}, device_id_type=MESH).wait_recv()
            cp = pltpu.make_async_remote_copy(block(buf, c, core), block(buf, c, core), gs_sem.at[r, 4 + n], gr_sem.at[r, 4 + n],
                                              device_id={"tp": sibling}, device_id_type=MESH)
            cp.start()
            second.append(cp)
        first[0].wait_recv()
        for cp in second:
            cp.wait_recv()
        return [*first.values(), *second]

    loads[0].wait()
    total, pending = scatter(0, a_ref, wo)
    if layer == 0:
        cx.wait()
        xrow = xs[...]
    else:
        xrow = x_in[...]
    xmid = (xrow.astype(F32) + total + bo_ref[...].astype(F32)[layer:layer + 1]).astype(BF16)
    pending += gather(0, hb, norm_rows(xmid.astype(F32), gain_ref[layer, 1:2, :], bias_ref[layer, 1:2, :]))
    loads[1].wait()
    up = jnp.dot(hb[...], wu[...], preferred_element_type=F32) + bu_ref[...].astype(F32)[layer:layer + 1]
    act[...] = jnp.maximum(up, 0.0).astype(BF16)
    loads[2].wait()
    total, started = scatter(1, act, wd)
    pending += started
    xnew = (xmid.astype(F32) + total + bd_ref[...].astype(F32)[layer:layer + 1]).astype(BF16)
    if last:
        rows = xnew
    else:
        xrow_out[...] = xnew
        rows = norm_rows(xnew.astype(F32), gain_ref[layer + 1, 0:1, :], bias_ref[layer + 1, 0:1, :])
    pending += gather(1, ob, rows)
    out_ref[...] = ob[...]
    for cp in pending:
        cp.wait_send()


def tail(layer, last, a, x, gain, bias, b_out, b_up, b_down, w_out, w_up, w_down):
    nb = a.shape[0]
    width = w_out.shape[-1]
    hidden = w_up.shape[-1]
    cut = nb // 8
    vmem = pl.BlockSpec(memory_space=pltpu.VMEM)
    hbm = pl.BlockSpec(memory_space=pl.ANY)
    out_shape = [jax.ShapeDtypeStruct((nb, width), BF16)]
    if not last:
        out_shape.append(jax.ShapeDtypeStruct((cut, width), BF16))
    return pl.pallas_call(
        functools.partial(tail_kernel, layer, last),
        in_specs=[vmem, hbm if layer == 0 else vmem, vmem, vmem, vmem, vmem, vmem, hbm, hbm, hbm],
        out_specs=[vmem] * len(out_shape),
        out_shape=out_shape,
        scratch_shapes=[
            pltpu.VMEM(w_out.shape[1:], BF16), pltpu.VMEM(w_up.shape[1:], BF16), pltpu.VMEM(w_down.shape[1:], BF16),
            pltpu.VMEM((cut, width), BF16), pltpu.VMEM((nb, width), BF16), pltpu.VMEM((nb, width), BF16),
            pltpu.VMEM((nb, hidden), BF16), pltpu.VMEM((nb // 2, width), F32),
            pltpu.VMEM((2, nb // 2, width), BF16), pltpu.VMEM((2, nb // 2, width), BF16),
            pltpu.VMEM((2, 3, cut, width), BF16), pltpu.VMEM((2, 3, cut, width), BF16),
            pltpu.SemaphoreType.DMA((3,)), pltpu.SemaphoreType.DMA,
            pltpu.SemaphoreType.DMA((2, 4)), pltpu.SemaphoreType.DMA((2, 4)),
            pltpu.SemaphoreType.DMA((2, 3)), pltpu.SemaphoreType.DMA((2, 3)),
            pltpu.SemaphoreType.DMA((2, 7)), pltpu.SemaphoreType.DMA((2, 7))],
        compiler_params=pltpu.CompilerParams(collective_id=layer, has_side_effects=True, vmem_limit_bytes=63 * 2 ** 20),
        cost_estimate=pl.CostEstimate(flops=10 ** 9, bytes_accessed=2 ** 22, transcendentals=0),
        name=f"tail_{layer}",
    )(a, x, gain, bias, b_out, b_up, b_down, w_out, w_up, w_down)


def solution(mesh):
    cache_spec = P(None, 'dp', 'tp', None, None)
    in_specs = (P('dp', None), P('dp'), cache_spec, cache_spec, P(), P(),
                P(None, None, None, 'tp', None), P(None, None, 'tp', None),
                P(None, 'tp', None, None), P(), P(None, None, 'tp'), P(None, 'tp'),
                P(None, 'tp', None), P())
    out_specs = (P('dp', None), cache_spec, cache_spec)

    def local_step(x, cache_len, k_cache, v_cache, norm_gain, norm_bias, w_qkv, b_qkv, w_out, b_out, w_up, b_up, w_down, b_down):
        layers = k_cache.shape[0]
        width = x.shape[1]
        k_t, v_t = k_cache.swapaxes(3, 4), v_cache.swapaxes(3, 4)
        w_t = w_qkv.transpose(0, 2, 3, 4, 1).reshape(layers, -1, width)
        w_o = w_out.reshape(layers, -1, width)
        h, xrow, caches = x, x, None
        for layer in range(layers):
            last = layer == layers - 1
            *caches, att = attention(layer, cache_len, h, norm_gain, norm_bias, w_t, b_qkv, k_t, v_t, caches)
            outs = tail(layer, last, att, xrow, norm_gain, norm_bias, b_out, b_up, b_down, w_o, w_up, w_down)
            h = outs[0]
            if not last:
                xrow = outs[1]
        return h, caches[0].swapaxes(3, 4), caches[1].swapaxes(3, 4)

    return jax.shard_map(local_step, mesh=mesh, in_specs=in_specs, out_specs=out_specs, check_vma=False)
```

```python
import functools

import jax
import jax.numpy as jnp
from jax import lax
from jax.experimental import pallas as pl
from jax.experimental.pallas import tpu as pltpu
from jax.sharding import PartitionSpec as P

F32 = jnp.float32
BF16 = jnp.bfloat16
EPS = 1e-5
MESH = pl.DeviceIdType.MESH
GB = 32
ATTN_VMEM = 63 * 2 ** 20
EARLY = 4


def norm_rows(xf, gain, bias):
    mean = jnp.mean(xf, axis=-1, keepdims=True)
    cen = xf - mean
    var = jnp.mean(cen * cen, axis=-1, keepdims=True)
    return (cen * lax.rsqrt(var + EPS) * gain + bias).astype(BF16)


def nt_dot(a, b):
    return lax.dot_general(a, b, (((1,), (1,)), ((), ())), preferred_element_type=F32)


def attn_kernel(layer, aliased, len_hbm, gain_hbm, bias_hbm, bq_hbm, x_in, w_hbm, k_hbm, v_hbm, *rest):
    if aliased:
        rest = rest[2:]
    k_out, v_out, a_out, len_ref, gain_ref, bias_ref, bq_ref, h_s, w_s, k_s, v_s, q_s, kvt_s, a_ref, in_sem, out_sem, a_sem, first_sem = rest
    nb = h_s.shape[0]
    hd = 128
    smax = 128
    groups = nb // GB

    def rows(g):
        return pl.ds(g * GB, GB)

    def load(g):
        return [pltpu.make_async_copy(hbm.at[layer, rows(g)], buf.at[rows(g)], in_sem.at[t, g])
                for t, (hbm, buf) in enumerate(((k_hbm, k_s), (v_hbm, v_s)))]

    def save_a(g):
        return pltpu.make_async_copy(a_ref.at[rows(g)], a_out.at[rows(g)], a_sem.at[g])

    def save(g):
        return [pltpu.make_async_copy(buf.at[rows(g)], hbm.at[layer, rows(g)], out_sem.at[t, g])
                for t, (hbm, buf) in enumerate(((k_out, k_s), (v_out, v_s)))]

    pairs = [(x_in, h_s), (w_hbm.at[layer], w_s), (bq_hbm, bq_ref), (len_hbm, len_ref)]
    if layer == 0:
        pairs += [(gain_hbm, gain_ref), (bias_hbm, bias_ref)]
    first = [pltpu.make_async_copy(src, dst, first_sem.at[i]) for i, (src, dst) in enumerate(pairs)]
    for cp in first:
        cp.start()
    for g in range(EARLY):
        for cp in load(g):
            cp.start()
    for cp in first:
        cp.wait()
    for g in range(EARLY, groups):
        for cp in load(g):
            cp.start()
    if layer == 0:
        for r in range(0, nb, 64):
            h_s[r:r + 64] = norm_rows(h_s[r:r + 64].astype(F32), gain_ref[layer, 0:1, :], bias_ref[layer, 0:1, :])
    bq = bq_ref[layer].astype(F32)
    bq = jnp.concatenate([bq[t, j:j + 1] for t in range(3) for j in range(2)], axis=1)
    qkv = nt_dot(h_s[...], w_s[...]) + bq
    q_s[...] = qkv[:, :hd].astype(BF16)
    kvt = jnp.swapaxes(qkv[:, hd:], 0, 1).astype(BF16)
    for t in range(nb // 128):
        kvt_s[t] = kvt[:, t * 128:(t + 1) * 128]

    row = lax.broadcasted_iota(jnp.int32, (GB, smax), 0)
    lane = lax.broadcasted_iota(jnp.int32, (GB, smax), 1)
    row_b = row.astype(F32).astype(BF16)
    lane_b = lane.astype(F32).astype(BF16)
    lane_c = lane_b[:16]
    lane_h = lane // 64
    low_b = lane_b < 64
    zero = jnp.zeros((GB, hd), BF16)
    even2 = lax.rem(lax.broadcasted_iota(jnp.int32, (2 * GB, smax), 0), 2).astype(F32).astype(BF16) < 0.5
    pair_of = lax.rem(lax.broadcasted_iota(jnp.int32, (hd, 2 * GB), 1), GB) // 2

    def weigh(g, p):
        nil = jnp.zeros_like(p)
        weights = jnp.concatenate([jnp.where(even2, p, nil), jnp.where(even2, nil, p)], axis=1)
        v = v_s[rows(g)].reshape(GB // 2, 2, hd, smax)
        pairs = jnp.concatenate([v[:, 0], v[:, 1]], axis=2).reshape(GB // 2 * hd, 2 * smax)
        o = nt_dot(pairs, weights)
        acc = o[:hd]
        for i in range(1, GB // 2):
            acc = jnp.where(pair_of == i, o[i * hd:(i + 1) * hd], acc)
        acc = jnp.swapaxes(acc, 0, 1)
        a_ref[rows(g), :] = jnp.where(lane_h == 0, acc[:GB], acc[GB:]).astype(BF16)
        save_a(g).start()

    def probs(g, lens):
        q = q_s[rows(g), :]
        qh = [jnp.where(low_b, q, zero), jnp.where(low_b, zero, q)]
        qbd = jnp.concatenate(
            [jnp.concatenate([jnp.where(row_b == i, qh[h], zero) for i in range(GB)], axis=1) for h in range(2)], axis=0)
        s = jnp.dot(qbd, k_s[rows(g)].reshape(GB * hd, smax), preferred_element_type=F32) * 0.125
        lentile = jnp.zeros((GB, smax), jnp.int32)
        for i in range(GB):
            lentile = jnp.where(row == i, lens[i], lentile)
        seen = lane <= lentile
        s = jnp.where(jnp.concatenate([seen, seen], axis=0), s, -1e30)
        m = jnp.max(s, axis=-1, keepdims=True)
        ex = jnp.exp(s - m)
        return (ex / jnp.sum(ex, axis=-1, keepdims=True)).astype(BF16)

    def insert(g, lens):
        for i in range(GB):
            b = g * GB + i
            hit = lane_c == lens[i].astype(F32).astype(BF16)
            shift = lax.rem(lens[i] - b % 128 + 128, 128)
            for part, buf in ((0, k_s), (1, v_s)):
                moved = pltpu.roll(kvt_s[b // 128, part * hd:(part + 1) * hd, :], shift, 1)
                old = buf[b].reshape(hd // 16, 16, smax)
                buf[b] = jnp.where(hit[None], moved.reshape(hd // 16, 16, smax), old).reshape(2, 64, smax)

    lens, p = {}, {}
    for g in range(groups + 2):
        if g < groups:
            for cp in load(g):
                cp.wait()
            lens[g] = [len_ref[g * GB + i] for i in range(GB)]
        if g >= 2:
            weigh(g - 2, p.pop(g - 2))
        if 1 <= g <= groups:
            p[g - 1] = probs(g - 1, lens[g - 1])
        if g < groups:
            insert(g, lens[g])
            for cp in save(g):
                cp.start()
    for g in range(groups):
        for cp in save(g) + [save_a(g)]:
            cp.wait()


def attention(layer, cache_len, x, gain, bias, w_t, b_qkv, k_t, v_t, prev):
    nl, nb = k_t.shape[:2]
    hbm = pl.BlockSpec(memory_space=pltpu.HBM)
    in_specs = [hbm, hbm, hbm, hbm, hbm, hbm, hbm, hbm]
    operands = [cache_len, gain, bias, b_qkv, x, w_t, k_t, v_t]
    aliases = {}
    if prev is not None:
        in_specs += [hbm, hbm]
        operands += list(prev)
        aliases = {8: 0, 9: 1}
    groups = nb // GB
    return pl.pallas_call(
        functools.partial(attn_kernel, layer, prev is not None),
        in_specs=in_specs,
        out_specs=[hbm, hbm, hbm],
        out_shape=[jax.ShapeDtypeStruct(k_t.shape, BF16), jax.ShapeDtypeStruct(v_t.shape, BF16),
                   jax.ShapeDtypeStruct((nb, 128), BF16)],
        scratch_shapes=[
            pltpu.SMEM(cache_len.shape, jnp.int32), pltpu.VMEM(gain.shape, F32), pltpu.VMEM(bias.shape, F32), pltpu.VMEM(b_qkv.shape, BF16),
            pltpu.VMEM(x.shape, BF16), pltpu.VMEM(w_t.shape[1:], BF16),
            pltpu.VMEM(k_t.shape[1:], BF16), pltpu.VMEM(v_t.shape[1:], BF16),
            pltpu.VMEM((nb, 128), BF16), pltpu.VMEM((nb // 128, 256, 128), BF16), pltpu.VMEM((nb, 128), BF16),
            pltpu.SemaphoreType.DMA((2, groups)), pltpu.SemaphoreType.DMA((2, groups)), pltpu.SemaphoreType.DMA((groups,)), pltpu.SemaphoreType.DMA((6,))],
        input_output_aliases=aliases,
        compiler_params=pltpu.CompilerParams(vmem_limit_bytes=ATTN_VMEM),
        cost_estimate=pl.CostEstimate(flops=10 ** 9, bytes_accessed=2 ** 25, transcendentals=0),
        name=f"attention_{layer}",
    )(*operands)


def tail_kernel(layer, last, a_hbm, x_hbm, gain_hbm, bias_hbm, bo_hbm, bu_hbm, bd_hbm, wo_hbm, wu_hbm, wd_hbm, *rest):
    if last:
        out_hbm, *rest = rest
    else:
        out_hbm, xrow_out, *rest = rest
    (a_s, gain_ref, bias_ref, bo_ref, bu, bd_ref, wo, wu, wd, xs, bu_x, wu_x, wd_x, hb, ob, own, dsend, drecv, csend, crecv,
     w_sem, o_sem, xs_sem, xr_sem, ds_sem, dr_sem, cs_sem, cr_sem, hs_sem, hr_sem, gs_sem, gr_sem) = rest
    nb = ob.shape[0]
    me = lax.axis_index("tp")
    core = lax.rem(me, 2)
    chip = lax.div(me, 2)
    half = nb // 2
    cut = nb // 8
    far = (3, 1, 2)

    def chip_at(dist):
        xb, yb = lax.rem(chip, 2), lax.div(chip, 2)
        dx, dy = dist % 2, dist // 2
        return (yb + dy - 2 * dy * yb) * 2 + xb + dx - 2 * dx * xb

    sibling = chip * 2 + 1 - core
    peers = {d: chip_at(d) * 2 + core for d in far}

    def send(src, dst, s_sem, r_sem, dev):
        return pltpu.make_async_remote_copy(src, dst, s_sem, r_sem, device_id={"tp": dev}, device_id_type=MESH)

    def slot(d):
        return pl.ds(pl.multiple_of(chip_at(d) * cut, cut), cut)

    row0 = pl.multiple_of(core * half + chip * cut, cut)
    x_mine = x_hbm.at[pl.ds(row0, cut)] if layer == 0 else x_hbm
    pairs = [(a_hbm, a_s), (wo_hbm.at[layer], wo), (x_mine, xs), (gain_hbm, gain_ref), (bias_hbm, bias_ref), (bo_hbm, bo_ref),
             (bu_hbm, bu), (bd_hbm, bd_ref), (wu_hbm.at[layer], wu), (wd_hbm.at[layer], wd)]
    loads = [pltpu.make_async_copy(src, dst, w_sem.at[i]) for i, (src, dst) in enumerate(pairs)]
    for cp in loads:
        cp.start()
    barrier = pltpu.get_barrier_semaphore()
    for dev in [sibling] + [peers[d] for d in far]:
        pl.semaphore_signal(barrier, inc=1, device_id={"tp": dev}, device_id_type=MESH)

    for cp in loads[:2]:
        cp.wait()
    dsend[...] = jnp.dot(a_s[pl.ds(pl.multiple_of((1 - core) * half, half), half), :], wo[...], preferred_element_type=F32).astype(BF16)
    pl.semaphore_wait(barrier, 4)
    d2d = {d: send(dsend.at[slot(d)], drecv.at[slot(d)], ds_sem.at[n], dr_sem.at[n], sibling) for n, d in enumerate(far + (0,))}
    for d in far + (0,):
        d2d[d].start()
    swap = [send(src, dst, xs_sem.at[n], xr_sem.at[n], sibling)
            for n, (src, dst) in enumerate(((bu_hbm, bu_x), (wu_hbm.at[layer], wu_x), (wd_hbm.at[layer], wd_x)))]
    for cp in swap:
        cp.start()
    own[...] = jnp.dot(a_s[pl.ds(pl.multiple_of(core * half, half), half), :], wo[...], preferred_element_type=F32)
    sends = {}
    for n, d in enumerate(far):
        d2d[d].wait_recv()
        csend[0, n] = (own[slot(d), :] + drecv[slot(d), :].astype(F32)).astype(BF16)
        sends[0, d] = send(csend.at[0, n], crecv.at[0, n], cs_sem.at[0, n], cr_sem.at[0, n], peers[d])
        sends[0, d].start()
    d2d[0].wait_recv()
    total = own[slot(0), :] + drecv[slot(0), :].astype(F32)
    for cp in loads[2:]:
        cp.wait()
    for n, d in ((2, 2), (1, 1), (0, 3)):
        sends[0, d].wait_recv()
        total = total + crecv[0, n].astype(F32)
    xmid = (xs[...].astype(F32) + total + bo_ref[...].astype(F32)[layer:layer + 1]).astype(BF16)

    hb[slot(0), :] = norm_rows(xmid.astype(F32), gain_ref[layer, 1:2, :], bias_ref[layer, 1:2, :])
    hsend = {d: send(hb.at[slot(0)], hb.at[slot(0)], hs_sem.at[n], hr_sem.at[n], peers[d]) for n, d in enumerate(far)}
    for d in far:
        hsend[d].start()
    for cp in swap:
        cp.wait_recv()

    def mlp(h):
        part = None
        for b_ref, u_ref, w_ref in ((bu, wu, wd), (bu_x, wu_x, wd_x)):
            up = jnp.dot(h, u_ref[...], preferred_element_type=F32) + b_ref[...].astype(F32)[layer:layer + 1]
            y = jnp.dot(jnp.maximum(up, 0.0).astype(BF16), w_ref[...], preferred_element_type=F32)
            part = y if part is None else part + y
        return part

    def arrived(d):
        n = far.index(d)
        send(hb.at[slot(0)], hb.at[slot(d)], hs_sem.at[n], hr_sem.at[n], peers[d]).wait_recv()

    total = mlp(hb[slot(0), :])
    for together in ((2, 3), (1,)):
        for d in together:
            arrived(d)
        part = mlp(jnp.concatenate([hb[slot(d), :] for d in together], axis=0))
        for i, d in sorted(enumerate(together), key=lambda t: -t[1]):
            n = far.index(d)
            csend[1, n] = part[i * cut:(i + 1) * cut].astype(BF16)
            sends[1, d] = send(csend.at[1, n], crecv.at[1, n], cs_sem.at[1, n], cr_sem.at[1, n], peers[d])
            sends[1, d].start()
    for n, d in ((2, 2), (0, 3), (1, 1)):
        sends[1, d].wait_recv()
        total = total + crecv[1, n].astype(F32)
    xnew = (xmid.astype(F32) + total + bd_ref[...].astype(F32)[layer:layer + 1]).astype(BF16)

    def block(d, k):
        return ob.at[pl.ds(pl.multiple_of(k * half + chip_at(d) * cut, cut), cut)]

    def keep(d, k, n):
        cp = pltpu.make_async_copy(block(d, k), out_hbm.at[pl.ds(pl.multiple_of(k * half + chip_at(d) * cut, cut), cut)], o_sem.at[n])
        cp.start()
        return cp

    mine = block(0, core)
    if last:
        mine[...] = xnew
    else:
        mine[...] = norm_rows(xnew.astype(F32), gain_ref[layer + 1, 0:1, :], bias_ref[layer + 1, 0:1, :])
    spread = {d: send(mine, mine, gs_sem.at[n], gr_sem.at[n], dev) for n, (d, dev) in enumerate([(d, peers[d]) for d in far] + [(0, sibling)])}
    for d in far + (0,):
        spread[d].start()
    kept = [keep(0, core, 0)]
    if not last:
        xs[...] = xnew
        kept.append(pltpu.make_async_copy(xs, xrow_out, o_sem.at[8]))
        kept[-1].start()
    passed = {}
    for d in (2, 3, 1):
        n = far.index(d)
        send(mine, block(d, core), gs_sem.at[n], gr_sem.at[n], peers[d]).wait_recv()
        passed[d] = send(block(d, core), block(d, core), gs_sem.at[4 + n], gr_sem.at[4 + n], sibling)
        passed[d].start()
        kept.append(keep(d, core, 1 + n))
    spread[0].wait_recv()
    kept.append(keep(0, 1 - core, 4))
    for d in (2, 3, 1):
        passed[d].wait_recv()
        kept.append(keep(d, 1 - core, 5 + far.index(d)))
    for cp in [*d2d.values(), *swap, *sends.values(), *hsend.values(), *spread.values(), *passed.values()]:
        cp.wait_send()
    for cp in kept:
        cp.wait()


def tail(layer, last, a, x, gain, bias, b_out, b_up, b_down, w_out, w_up, w_down):
    nb = a.shape[0]
    width = w_out.shape[-1]
    half, cut = nb // 2, nb // 8
    hbm = pl.BlockSpec(memory_space=pltpu.HBM)
    out_shape = [jax.ShapeDtypeStruct((nb, width), BF16)]
    if not last:
        out_shape.append(jax.ShapeDtypeStruct((cut, width), BF16))
    dma = pltpu.SemaphoreType.DMA
    return pl.pallas_call(
        functools.partial(tail_kernel, layer, last),
        in_specs=[hbm] * 10,
        out_specs=[hbm] * len(out_shape),
        out_shape=out_shape,
        scratch_shapes=[
            pltpu.VMEM(a.shape, BF16), pltpu.VMEM(gain.shape, F32), pltpu.VMEM(bias.shape, F32),
            pltpu.VMEM(b_out.shape, BF16), pltpu.VMEM(b_up.shape, BF16), pltpu.VMEM(b_down.shape, BF16),
            pltpu.VMEM(w_out.shape[1:], BF16), pltpu.VMEM(w_up.shape[1:], BF16), pltpu.VMEM(w_down.shape[1:], BF16),
            pltpu.VMEM((cut, width), BF16),
            pltpu.VMEM(b_up.shape, BF16), pltpu.VMEM(w_up.shape[1:], BF16), pltpu.VMEM(w_down.shape[1:], BF16),
            pltpu.VMEM((half, width), BF16), pltpu.VMEM((nb, width), BF16), pltpu.VMEM((half, width), F32),
            pltpu.VMEM((half, width), BF16), pltpu.VMEM((half, width), BF16),
            pltpu.VMEM((2, 3, cut, width), BF16), pltpu.VMEM((2, 3, cut, width), BF16),
            dma((10,)), dma((9,)), dma((3,)), dma((3,)), dma((4,)), dma((4,)),
            dma((2, 3)), dma((2, 3)), dma((3,)), dma((3,)), dma((7,)), dma((7,))],
        compiler_params=pltpu.CompilerParams(collective_id=layer, has_side_effects=True, vmem_limit_bytes=ATTN_VMEM),
        cost_estimate=pl.CostEstimate(flops=10 ** 9, bytes_accessed=2 ** 22, transcendentals=0),
        name=f"tail_{layer}",
    )(a, x, gain, bias, b_out, b_up, b_down, w_out, w_up, w_down)


def solution(mesh):
    cache_spec = P(None, 'dp', 'tp', None, None)
    in_specs = (P('dp', None), P('dp'), cache_spec, cache_spec, P(), P(),
                P(None, None, None, 'tp', None), P(None, None, 'tp', None),
                P(None, 'tp', None, None), P(), P(None, None, 'tp'), P(None, 'tp'),
                P(None, 'tp', None), P())
    out_specs = (P('dp', None), cache_spec, cache_spec)

    def local_step(x, cache_len, k_cache, v_cache, norm_gain, norm_bias, w_qkv, b_qkv, w_out, b_out, w_up, b_up, w_down, b_down):
        layers = k_cache.shape[0]
        width = x.shape[1]
        k_t, v_t = k_cache.swapaxes(3, 4), v_cache.swapaxes(3, 4)
        w_t = w_qkv.transpose(0, 2, 3, 4, 1).reshape(layers, -1, width)
        w_o = w_out.reshape(layers, -1, width)
        h, xrow, caches = x, x, None
        for layer in range(layers):
            last = layer == layers - 1
            *caches, att = attention(layer, cache_len, h, norm_gain, norm_bias, w_t, b_qkv, k_t, v_t, caches)
            outs = tail(layer, last, att, xrow, norm_gain, norm_bias, b_out, b_up, b_down, w_o, w_up, w_down)
            h = outs[0]
            if not last:
                xrow = outs[1]
        return h, caches[0].swapaxes(3, 4), caches[1].swapaxes(3, 4)

    return jax.shard_map(local_step, mesh=mesh, in_specs=in_specs, out_specs=out_specs, check_vma=False)
```

```python
import functools

import jax
import jax.numpy as jnp
from jax import lax
from jax.experimental import pallas as pl
from jax.experimental.pallas import tpu as pltpu
from jax.sharding import PartitionSpec as P

F32 = jnp.float32
BF16 = jnp.bfloat16
EPS = 1e-5
MESH = pl.DeviceIdType.MESH
GB = 32
ATTN_VMEM = 63 * 2 ** 20
EARLY = 4


def norm_rows(xf, gain, bias):
    mean = jnp.mean(xf, axis=-1, keepdims=True)
    cen = xf - mean
    var = jnp.mean(cen * cen, axis=-1, keepdims=True)
    return (cen * lax.rsqrt(var + EPS) * gain + bias).astype(BF16)


def nt_dot(a, b):
    return lax.dot_general(a, b, (((1,), (1,)), ((), ())), preferred_element_type=F32)


def attn_kernel(layer, aliased, len_hbm, gain_hbm, bias_hbm, bq_hbm, x_in, w_hbm, k_hbm, v_hbm, *rest):
    if aliased:
        rest = rest[2:]
    k_out, v_out, a_out, len_ref, gain_ref, bias_ref, bq_ref, h_s, w_s, k_s, v_s, q_s, kvt_s, a_ref, in_sem, out_sem, a_sem, first_sem = rest
    nb = h_s.shape[0]
    hd = 128
    smax = 128
    groups = nb // GB

    def rows(g):
        return pl.ds(g * GB, GB)

    def load(g):
        return [pltpu.make_async_copy(hbm.at[layer, rows(g)], buf.at[rows(g)], in_sem.at[t, g])
                for t, (hbm, buf) in enumerate(((k_hbm, k_s), (v_hbm, v_s)))]

    def save_a(g):
        return pltpu.make_async_copy(a_ref.at[rows(g)], a_out.at[rows(g)], a_sem.at[g])

    def save(g):
        return [pltpu.make_async_copy(buf.at[rows(g)], hbm.at[layer, rows(g)], out_sem.at[t, g])
                for t, (hbm, buf) in enumerate(((k_out, k_s), (v_out, v_s)))]

    pairs = [(x_in, h_s), (w_hbm.at[layer], w_s), (bq_hbm, bq_ref), (len_hbm, len_ref)]
    if layer == 0:
        pairs += [(gain_hbm, gain_ref), (bias_hbm, bias_ref)]
    first = [pltpu.make_async_copy(src, dst, first_sem.at[i]) for i, (src, dst) in enumerate(pairs)]
    for cp in first:
        cp.start()
    for g in range(EARLY):
        for cp in load(g):
            cp.start()
    for cp in first:
        cp.wait()
    for g in range(EARLY, groups):
        for cp in load(g):
            cp.start()
    if layer == 0:
        for r in range(0, nb, 64):
            h_s[r:r + 64] = norm_rows(h_s[r:r + 64].astype(F32), gain_ref[layer, 0:1, :], bias_ref[layer, 0:1, :])
    bq = bq_ref[layer].astype(F32)
    bq = jnp.concatenate([bq[t, j:j + 1] for t in range(3) for j in range(2)], axis=1)
    qkv = nt_dot(h_s[...], w_s[...]) + bq
    q_s[...] = qkv[:, :hd].astype(BF16)
    kvt = jnp.swapaxes(qkv[:, hd:], 0, 1).astype(BF16)
    for t in range(nb // 128):
        kvt_s[t] = kvt[:, t * 128:(t + 1) * 128]

    row = lax.broadcasted_iota(jnp.int32, (GB, smax), 0)
    lane = lax.broadcasted_iota(jnp.int32, (GB, smax), 1)
    row_b = row.astype(F32).astype(BF16)
    lane_b = lane.astype(F32).astype(BF16)
    lane_c = lane_b[:16]
    lane_h = lane // 64
    low_b = lane_b < 64
    zero = jnp.zeros((GB, hd), BF16)
    even2 = lax.rem(lax.broadcasted_iota(jnp.int32, (2 * GB, smax), 0), 2).astype(F32).astype(BF16) < 0.5
    pair_of = lax.rem(lax.broadcasted_iota(jnp.int32, (hd, 2 * GB), 1), GB) // 2

    def weigh(g, p):
        nil = jnp.zeros_like(p)
        weights = jnp.concatenate([jnp.where(even2, p, nil), jnp.where(even2, nil, p)], axis=1)
        v = v_s[rows(g)].reshape(GB // 2, 2, hd, smax)
        pairs = jnp.concatenate([v[:, 0], v[:, 1]], axis=2).reshape(GB // 2 * hd, 2 * smax)
        o = nt_dot(pairs, weights)
        acc = o[:hd]
        for i in range(1, GB // 2):
            acc = jnp.where(pair_of == i, o[i * hd:(i + 1) * hd], acc)
        acc = jnp.swapaxes(acc, 0, 1)
        a_ref[rows(g), :] = jnp.where(lane_h == 0, acc[:GB], acc[GB:]).astype(BF16)
        save_a(g).start()

    def probs(g, lens):
        q = q_s[rows(g), :]
        qh = [jnp.where(low_b, q, zero), jnp.where(low_b, zero, q)]
        qbd = jnp.concatenate(
            [jnp.concatenate([jnp.where(row_b == i, qh[h], zero) for i in range(GB)], axis=1) for h in range(2)], axis=0)
        s = jnp.dot(qbd, k_s[rows(g)].reshape(GB * hd, smax), preferred_element_type=F32) * 0.125
        lentile = jnp.zeros((GB, smax), jnp.int32)
        for i in range(GB):
            lentile = jnp.where(row == i, lens[i], lentile)
        seen = lane <= lentile
        s = jnp.where(jnp.concatenate([seen, seen], axis=0), s, -1e30)
        m = jnp.max(s, axis=-1, keepdims=True)
        ex = jnp.exp(s - m)
        return (ex / jnp.sum(ex, axis=-1, keepdims=True)).astype(BF16)

    def insert(g, lens):
        for i in range(GB):
            b = g * GB + i
            hit = lane_c == lens[i].astype(F32).astype(BF16)
            shift = lax.rem(lens[i] - b % 128 + 128, 128)
            for part, buf in ((0, k_s), (1, v_s)):
                moved = pltpu.roll(kvt_s[b // 128, part * hd:(part + 1) * hd, :], shift, 1)
                old = buf[b].reshape(hd // 16, 16, smax)
                buf[b] = jnp.where(hit[None], moved.reshape(hd // 16, 16, smax), old).reshape(2, 64, smax)

    lens, p = {}, {}
    for g in range(groups + 2):
        if g < groups:
            for cp in load(g):
                cp.wait()
            lens[g] = [len_ref[g * GB + i] for i in range(GB)]
        if g >= 2:
            weigh(g - 2, p.pop(g - 2))
        if 1 <= g <= groups:
            p[g - 1] = probs(g - 1, lens[g - 1])
        if g < groups:
            insert(g, lens[g])
            for cp in save(g):
                cp.start()
    for g in range(groups):
        for cp in save(g) + [save_a(g)]:
            cp.wait()


def attention(layer, cache_len, x, gain, bias, w_t, b_qkv, k_t, v_t, prev):
    nl, nb = k_t.shape[:2]
    hbm = pl.BlockSpec(memory_space=pltpu.HBM)
    in_specs = [hbm, hbm, hbm, hbm, hbm, hbm, hbm, hbm]
    operands = [cache_len, gain, bias, b_qkv, x, w_t, k_t, v_t]
    aliases = {}
    if prev is not None:
        in_specs += [hbm, hbm]
        operands += list(prev)
        aliases = {8: 0, 9: 1}
    groups = nb // GB
    return pl.pallas_call(
        functools.partial(attn_kernel, layer, prev is not None),
        in_specs=in_specs,
        out_specs=[hbm, hbm, hbm],
        out_shape=[jax.ShapeDtypeStruct(k_t.shape, BF16), jax.ShapeDtypeStruct(v_t.shape, BF16),
                   jax.ShapeDtypeStruct((nb, 128), BF16)],
        scratch_shapes=[
            pltpu.SMEM(cache_len.shape, jnp.int32), pltpu.VMEM(gain.shape, F32), pltpu.VMEM(bias.shape, F32), pltpu.VMEM(b_qkv.shape, BF16),
            pltpu.VMEM(x.shape, BF16), pltpu.VMEM(w_t.shape[1:], BF16),
            pltpu.VMEM(k_t.shape[1:], BF16), pltpu.VMEM(v_t.shape[1:], BF16),
            pltpu.VMEM((nb, 128), BF16), pltpu.VMEM((nb // 128, 256, 128), BF16), pltpu.VMEM((nb, 128), BF16),
            pltpu.SemaphoreType.DMA((2, groups)), pltpu.SemaphoreType.DMA((2, groups)), pltpu.SemaphoreType.DMA((groups,)), pltpu.SemaphoreType.DMA((6,))],
        input_output_aliases=aliases,
        compiler_params=pltpu.CompilerParams(vmem_limit_bytes=ATTN_VMEM),
        cost_estimate=pl.CostEstimate(flops=10 ** 9, bytes_accessed=2 ** 25, transcendentals=0),
        name=f"attention_{layer}",
    )(*operands)


PIECES = 2


def tail_kernel(layer, last, a_hbm, x_hbm, gain_hbm, bias_hbm, bo_hbm, bu_hbm, bd_hbm, wo_hbm, wu_hbm, wd_hbm, *rest):
    if last:
        out_hbm, *rest = rest
    else:
        out_hbm, xrow_out, *rest = rest
    (a_s, gain_ref, bias_ref, bo_ref, bu, bd_ref, wo, wu, wd, xs, bu_x, wu_x, wd_x, hb, ob, own, dsend, drecv, csend, crecv,
     w_sem, o_sem, xs_sem, xr_sem, ds_sem, dr_sem, cs_sem, cr_sem, hs_sem, hr_sem, gs_sem, gr_sem) = rest
    nb = ob.shape[0]
    me = lax.axis_index("tp")
    core = lax.rem(me, 2)
    chip = lax.div(me, 2)
    half = nb // 2
    cut = nb // 8
    piece = cut // PIECES
    pieces = range(PIECES)
    far = (3, 1, 2)

    def chip_at(dist):
        xb, yb = lax.rem(chip, 2), lax.div(chip, 2)
        dx, dy = dist % 2, dist // 2
        return (yb + dy - 2 * dy * yb) * 2 + xb + dx - 2 * dx * xb

    sibling = chip * 2 + 1 - core
    peers = {d: chip_at(d) * 2 + core for d in far}

    def send(src, dst, s_sem, r_sem, dev):
        return pltpu.make_async_remote_copy(src, dst, s_sem, r_sem, device_id={"tp": dev}, device_id_type=MESH)

    def slot(d, s):
        return pl.ds(pl.multiple_of(chip_at(d) * cut + s * piece, piece), piece)

    def at(s):
        return pl.ds(s * piece, piece)

    row0 = pl.multiple_of(core * half + chip * cut, cut)
    x_mine = x_hbm.at[pl.ds(row0, cut)] if layer == 0 else x_hbm
    pairs = [(a_hbm, a_s), (wo_hbm.at[layer], wo), (x_mine, xs), (gain_hbm, gain_ref), (bias_hbm, bias_ref), (bo_hbm, bo_ref),
             (bu_hbm, bu), (bd_hbm, bd_ref), (wu_hbm.at[layer], wu), (wd_hbm.at[layer], wd)]
    loads = [pltpu.make_async_copy(src, dst, w_sem.at[i]) for i, (src, dst) in enumerate(pairs)]
    for cp in loads:
        cp.start()
    barrier = pltpu.get_barrier_semaphore()
    for dev in [sibling] + [peers[d] for d in far]:
        pl.semaphore_signal(barrier, inc=1, device_id={"tp": dev}, device_id_type=MESH)

    for cp in loads[:2]:
        cp.wait()
    dsend[...] = jnp.dot(a_s[pl.ds(pl.multiple_of((1 - core) * half, half), half), :], wo[...], preferred_element_type=F32).astype(BF16)
    pl.semaphore_wait(barrier, 4)
    d2d = {(s, d): send(dsend.at[slot(d, s)], drecv.at[slot(d, s)], ds_sem.at[s, n], dr_sem.at[s, n], sibling)
           for s in pieces for n, d in enumerate(far + (0,))}
    for cp in d2d.values():
        cp.start()
    swap = [send(src, dst, xs_sem.at[n], xr_sem.at[n], sibling)
            for n, (src, dst) in enumerate(((bu_hbm, bu_x), (wu_hbm.at[layer], wu_x), (wd_hbm.at[layer], wd_x)))]
    for cp in swap:
        cp.start()
    own[...] = jnp.dot(a_s[pl.ds(pl.multiple_of(core * half, half), half), :], wo[...], preferred_element_type=F32)
    sends = {}

    def reduce_to(r, s, d, part):
        n = far.index(d)
        csend[r, n, at(s), :] = part.astype(BF16)
        sends[r, s, d] = send(csend.at[r, n, at(s)], crecv.at[r, n, at(s)], cs_sem.at[r, s, n], cr_sem.at[r, s, n], peers[d])
        sends[r, s, d].start()

    def received(r, s, total):
        for d in (2, 3, 1):
            sends[r, s, d].wait_recv()
            total = total + crecv[r, far.index(d), at(s), :].astype(F32)
        return total

    for s in pieces:
        for d in far:
            d2d[s, d].wait_recv()
            reduce_to(0, s, d, own[slot(d, s), :] + drecv[slot(d, s), :].astype(F32))
    for cp in loads[2:]:
        cp.wait()
    xmid, hsend = {}, {}
    for s in pieces:
        d2d[s, 0].wait_recv()
        total = received(0, s, own[slot(0, s), :] + drecv[slot(0, s), :].astype(F32))
        xmid[s] = (xs[at(s), :].astype(F32) + total + bo_ref[...].astype(F32)[layer:layer + 1]).astype(BF16)
        mine = hb.at[slot(0, s)]
        mine[...] = norm_rows(xmid[s].astype(F32), gain_ref[layer, 1:2, :], bias_ref[layer, 1:2, :])
        for n, d in enumerate(far):
            hsend[s, d] = send(mine, mine, hs_sem.at[s, n], hr_sem.at[s, n], peers[d])
            hsend[s, d].start()

    for cp in swap:
        cp.wait_recv()

    def mlp(h):
        part = None
        for b_ref, u_ref, w_ref in ((bu, wu, wd), (bu_x, wu_x, wd_x)):
            up = jnp.dot(h, u_ref[...], preferred_element_type=F32) + b_ref[...].astype(F32)[layer:layer + 1]
            y = jnp.dot(jnp.maximum(up, 0.0).astype(BF16), w_ref[...], preferred_element_type=F32)
            part = y if part is None else part + y
        return part

    own[0:cut, :] = mlp(jnp.concatenate([hb[slot(0, s), :] for s in pieces], axis=0))
    for s in pieces:
        for n, d in enumerate(far):
            send(hb.at[slot(0, s)], hb.at[slot(d, s)], hs_sem.at[s, n], hr_sem.at[s, n], peers[d]).wait_recv()
        part = mlp(jnp.concatenate([hb[slot(d, s), :] for d in far], axis=0))
        for n, d in enumerate(far):
            reduce_to(1, s, d, part[n * piece:(n + 1) * piece])

    def place(d, k, s):
        return pl.ds(pl.multiple_of(k * half + chip_at(d) * cut + s * piece, piece), piece)

    kept = []

    def keep(d, k, s, n):
        kept.append(pltpu.make_async_copy(ob.at[place(d, k, s)], out_hbm.at[place(d, k, s)], o_sem.at[s, n]))
        kept[-1].start()

    spread = {}
    for s in pieces:
        total = received(1, s, own[at(s), :])
        xnew = (xmid[s].astype(F32) + total + bd_ref[...].astype(F32)[layer:layer + 1]).astype(BF16)
        mine = ob.at[place(0, core, s)]
        if last:
            mine[...] = xnew
        else:
            mine[...] = norm_rows(xnew.astype(F32), gain_ref[layer + 1, 0:1, :], bias_ref[layer + 1, 0:1, :])
        for n, (d, dev) in enumerate([(d, peers[d]) for d in far] + [(0, sibling)]):
            spread[s, d] = send(mine, mine, gs_sem.at[s, n], gr_sem.at[s, n], dev)
            spread[s, d].start()
        keep(0, core, s, 0)
        if not last:
            xs[at(s), :] = xnew
            kept.append(pltpu.make_async_copy(xs.at[at(s)], xrow_out.at[at(s)], o_sem.at[s, 8]))
            kept[-1].start()
    passed = {}
    for s in pieces:
        for d in (2, 3, 1):
            n = far.index(d)
            block = ob.at[place(d, core, s)]
            send(ob.at[place(0, core, s)], block, gs_sem.at[s, n], gr_sem.at[s, n], peers[d]).wait_recv()
            passed[s, d] = send(block, block, gs_sem.at[s, 4 + n], gr_sem.at[s, 4 + n], sibling)
            passed[s, d].start()
            keep(d, core, s, 1 + n)
    for s in pieces:
        spread[s, 0].wait_recv()
        keep(0, 1 - core, s, 4)
        for d in (2, 3, 1):
            passed[s, d].wait_recv()
            keep(d, 1 - core, s, 5 + far.index(d))
    for cp in [*d2d.values(), *swap, *sends.values(), *hsend.values(), *spread.values(), *passed.values()]:
        cp.wait_send()
    for cp in kept:
        cp.wait()


def tail(layer, last, a, x, gain, bias, b_out, b_up, b_down, w_out, w_up, w_down):
    nb = a.shape[0]
    width = w_out.shape[-1]
    half, cut = nb // 2, nb // 8
    hbm = pl.BlockSpec(memory_space=pltpu.HBM)
    out_shape = [jax.ShapeDtypeStruct((nb, width), BF16)]
    if not last:
        out_shape.append(jax.ShapeDtypeStruct((cut, width), BF16))
    dma = pltpu.SemaphoreType.DMA
    return pl.pallas_call(
        functools.partial(tail_kernel, layer, last),
        in_specs=[hbm] * 10,
        out_specs=[hbm] * len(out_shape),
        out_shape=out_shape,
        scratch_shapes=[
            pltpu.VMEM(a.shape, BF16), pltpu.VMEM(gain.shape, F32), pltpu.VMEM(bias.shape, F32),
            pltpu.VMEM(b_out.shape, BF16), pltpu.VMEM(b_up.shape, BF16), pltpu.VMEM(b_down.shape, BF16),
            pltpu.VMEM(w_out.shape[1:], BF16), pltpu.VMEM(w_up.shape[1:], BF16), pltpu.VMEM(w_down.shape[1:], BF16),
            pltpu.VMEM((cut, width), BF16),
            pltpu.VMEM(b_up.shape, BF16), pltpu.VMEM(w_up.shape[1:], BF16), pltpu.VMEM(w_down.shape[1:], BF16),
            pltpu.VMEM((half, width), BF16), pltpu.VMEM((nb, width), BF16), pltpu.VMEM((half, width), F32),
            pltpu.VMEM((half, width), BF16), pltpu.VMEM((half, width), BF16),
            pltpu.VMEM((2, 3, cut, width), BF16), pltpu.VMEM((2, 3, cut, width), BF16),
            dma((10,)), dma((PIECES, 9)), dma((3,)), dma((3,)), dma((PIECES, 4)), dma((PIECES, 4)),
            dma((2, PIECES, 3)), dma((2, PIECES, 3)), dma((PIECES, 3)), dma((PIECES, 3)), dma((PIECES, 7)), dma((PIECES, 7))],
        compiler_params=pltpu.CompilerParams(collective_id=layer, has_side_effects=True, vmem_limit_bytes=ATTN_VMEM),
        cost_estimate=pl.CostEstimate(flops=10 ** 9, bytes_accessed=2 ** 22, transcendentals=0),
        name=f"tail_{layer}",
    )(a, x, gain, bias, b_out, b_up, b_down, w_out, w_up, w_down)


def solution(mesh):
    cache_spec = P(None, 'dp', 'tp', None, None)
    in_specs = (P('dp', None), P('dp'), cache_spec, cache_spec, P(), P(),
                P(None, None, None, 'tp', None), P(None, None, 'tp', None),
                P(None, 'tp', None, None), P(), P(None, None, 'tp'), P(None, 'tp'),
                P(None, 'tp', None), P())
    out_specs = (P('dp', None), cache_spec, cache_spec)

    def local_step(x, cache_len, k_cache, v_cache, norm_gain, norm_bias, w_qkv, b_qkv, w_out, b_out, w_up, b_up, w_down, b_down):
        layers = k_cache.shape[0]
        width = x.shape[1]
        k_t, v_t = k_cache.swapaxes(3, 4), v_cache.swapaxes(3, 4)
        w_t = w_qkv.transpose(0, 2, 3, 4, 1).reshape(layers, -1, width)
        w_o = w_out.reshape(layers, -1, width)
        h, xrow, caches = x, x, None
        for layer in range(layers):
            last = layer == layers - 1
            *caches, att = attention(layer, cache_len, h, norm_gain, norm_bias, w_t, b_qkv, k_t, v_t, caches)
            outs = tail(layer, last, att, xrow, norm_gain, norm_bias, b_out, b_up, b_down, w_o, w_up, w_down)
            h = outs[0]
            if not last:
                xrow = outs[1]
        return h, caches[0].swapaxes(3, 4), caches[1].swapaxes(3, 4)

    return jax.shard_map(local_step, mesh=mesh, in_specs=in_specs, out_specs=out_specs, check_vma=False)
```

```python
import functools

import jax
import jax.numpy as jnp
from jax import lax
from jax.experimental import pallas as pl
from jax.experimental.pallas import tpu as pltpu
from jax.sharding import PartitionSpec as P

F32 = jnp.float32
BF16 = jnp.bfloat16
EPS = 1e-5
MESH = pl.DeviceIdType.MESH
GB = 32
ATTN_VMEM = 63 * 2 ** 20
READS = ((0, 1), (1, 2), (2, 4), (4, 6), (6, 8))
WRITES = (((0, 2), (2, 4), (4, 6), (6, 7), (7, 8)), ((0, 1), (1, 3), (3, 5), (5, 7), (7, 8)))
EARLY = 3


def norm_rows(xf, gain, bias):
    mean = jnp.mean(xf, axis=-1, keepdims=True)
    cen = xf - mean
    var = jnp.mean(cen * cen, axis=-1, keepdims=True)
    return (cen * lax.rsqrt(var + EPS) * gain + bias).astype(BF16)


def nt_dot(a, b):
    return lax.dot_general(a, b, (((1,), (1,)), ((), ())), preferred_element_type=F32)


def attn_kernel(layer, aliased, len_hbm, gain_hbm, bias_hbm, bq_hbm, x_in, w_hbm, k_hbm, v_hbm, *rest):
    if aliased:
        rest = rest[2:]
    k_out, v_out, a_out, len_ref, gain_ref, bias_ref, bq_ref, h_s, w_s, k_s, v_s, q_s, kvt_s, a_ref, in_sem, out_sem, a_sem, first_sem = rest
    nb = h_s.shape[0]
    hd = 128
    smax = 128
    groups = nb // GB

    def rows(g):
        return pl.ds(g * GB, GB)

    def part(piece):
        return pl.ds(piece[0] * GB, (piece[1] - piece[0]) * GB)

    def load(piece):
        return [pltpu.make_async_copy(hbm.at[layer, part(piece)], buf.at[part(piece)], in_sem.at[t, piece[0]])
                for t, (hbm, buf) in enumerate(((k_hbm, k_s), (v_hbm, v_s)))]

    def save_a(g):
        return pltpu.make_async_copy(a_ref.at[rows(g)], a_out.at[rows(g)], a_sem.at[g])

    def save(piece):
        return [pltpu.make_async_copy(buf.at[part(piece)], hbm.at[layer, part(piece)], out_sem.at[t, piece[0]])
                for t, (hbm, buf) in enumerate(((k_out, k_s), (v_out, v_s)))]

    pairs = [(x_in, h_s), (w_hbm.at[layer], w_s), (bq_hbm, bq_ref), (len_hbm, len_ref)]
    if layer == 0:
        pairs += [(gain_hbm, gain_ref), (bias_hbm, bias_ref)]
    first = [pltpu.make_async_copy(src, dst, first_sem.at[i]) for i, (src, dst) in enumerate(pairs)]
    for cp in first:
        cp.start()
    for piece in READS[:EARLY]:
        for cp in load(piece):
            cp.start()
    for cp in first:
        cp.wait()
    for piece in READS[EARLY:]:
        for cp in load(piece):
            cp.start()
    if layer == 0:
        for r in range(0, nb, 64):
            h_s[r:r + 64] = norm_rows(h_s[r:r + 64].astype(F32), gain_ref[layer, 0:1, :], bias_ref[layer, 0:1, :])
    bq = bq_ref[layer].astype(F32)
    bq = jnp.concatenate([bq[t, j:j + 1] for t in range(3) for j in range(2)], axis=1)
    qkv = nt_dot(h_s[...], w_s[...]) + bq
    q_s[...] = qkv[:, :hd].astype(BF16)
    kvt = jnp.swapaxes(qkv[:, hd:], 0, 1).astype(BF16)
    for t in range(nb // 128):
        kvt_s[t] = kvt[:, t * 128:(t + 1) * 128]

    row = lax.broadcasted_iota(jnp.int32, (GB, smax), 0)
    lane = lax.broadcasted_iota(jnp.int32, (GB, smax), 1)
    row_b = row.astype(F32).astype(BF16)
    lane_b = lane.astype(F32).astype(BF16)
    lane_c = lane_b[:16]
    lane_h = lane // 64
    low_b = lane_b < 64
    zero = jnp.zeros((GB, hd), BF16)
    even2 = lax.rem(lax.broadcasted_iota(jnp.int32, (2 * GB, smax), 0), 2).astype(F32).astype(BF16) < 0.5
    pair_of = lax.rem(lax.broadcasted_iota(jnp.int32, (hd, 2 * GB), 1), GB) // 2

    def weigh(g, p):
        nil = jnp.zeros_like(p)
        weights = jnp.concatenate([jnp.where(even2, p, nil), jnp.where(even2, nil, p)], axis=1)
        v = v_s[rows(g)].reshape(GB // 2, 2, hd, smax)
        pairs = jnp.concatenate([v[:, 0], v[:, 1]], axis=2).reshape(GB // 2 * hd, 2 * smax)
        o = nt_dot(pairs, weights)
        acc = o[:hd]
        for i in range(1, GB // 2):
            acc = jnp.where(pair_of == i, o[i * hd:(i + 1) * hd], acc)
        acc = jnp.swapaxes(acc, 0, 1)
        a_ref[rows(g), :] = jnp.where(lane_h == 0, acc[:GB], acc[GB:]).astype(BF16)
        save_a(g).start()

    def probs(g, lens):
        q = q_s[rows(g), :]
        qh = [jnp.where(low_b, q, zero), jnp.where(low_b, zero, q)]
        qbd = jnp.concatenate(
            [jnp.concatenate([jnp.where(row_b == i, qh[h], zero) for i in range(GB)], axis=1) for h in range(2)], axis=0)
        s = jnp.dot(qbd, k_s[rows(g)].reshape(GB * hd, smax), preferred_element_type=F32) * 0.125
        lentile = jnp.zeros((GB, smax), jnp.int32)
        for i in range(GB):
            lentile = jnp.where(row == i, lens[i], lentile)
        seen = lane <= lentile
        s = jnp.where(jnp.concatenate([seen, seen], axis=0), s, -1e30)
        m = jnp.max(s, axis=-1, keepdims=True)
        ex = jnp.exp(s - m)
        return (ex / jnp.sum(ex, axis=-1, keepdims=True)).astype(BF16)

    def insert(g, lens):
        for i in range(GB):
            b = g * GB + i
            hit = lane_c == lens[i].astype(F32).astype(BF16)
            shift = lax.rem(lens[i] - b % 128 + 128, 128)
            for part, buf in ((0, k_s), (1, v_s)):
                moved = pltpu.roll(kvt_s[b // 128, part * hd:(part + 1) * hd, :], shift, 1)
                old = buf[b].reshape(hd // 16, 16, smax)
                buf[b] = jnp.where(hit[None], moved.reshape(hd // 16, 16, smax), old).reshape(2, 64, smax)

    lens, p = {}, {}
    for g in range(groups + 2):
        if g < groups:
            for piece in READS:
                if piece[0] == g:
                    for cp in load(piece):
                        cp.wait()
            lens[g] = [len_ref[g * GB + i] for i in range(GB)]
        if g >= 2:
            weigh(g - 2, p.pop(g - 2))
        if 1 <= g <= groups:
            p[g - 1] = probs(g - 1, lens[g - 1])
        if g < groups:
            insert(g, lens[g])
            for piece in WRITES[layer % 2]:
                if piece[1] == g + 1:
                    for cp in save(piece):
                        cp.start()
    for piece in WRITES[layer % 2]:
        for cp in save(piece):
            cp.wait()
    for g in range(groups):
        save_a(g).wait()


def attention(layer, cache_len, x, gain, bias, w_t, b_qkv, k_t, v_t, prev):
    nl, nb = k_t.shape[:2]
    hbm = pl.BlockSpec(memory_space=pltpu.HBM)
    in_specs = [hbm, hbm, hbm, hbm, hbm, hbm, hbm, hbm]
    operands = [cache_len, gain, bias, b_qkv, x, w_t, k_t, v_t]
    aliases = {}
    if prev is not None:
        in_specs += [hbm, hbm]
        operands += list(prev)
        aliases = {8: 0, 9: 1}
    groups = nb // GB
    return pl.pallas_call(
        functools.partial(attn_kernel, layer, prev is not None),
        in_specs=in_specs,
        out_specs=[hbm, hbm, hbm],
        out_shape=[jax.ShapeDtypeStruct(k_t.shape, BF16), jax.ShapeDtypeStruct(v_t.shape, BF16),
                   jax.ShapeDtypeStruct((nb, 128), BF16)],
        scratch_shapes=[
            pltpu.SMEM(cache_len.shape, jnp.int32), pltpu.VMEM(gain.shape, F32), pltpu.VMEM(bias.shape, F32), pltpu.VMEM(b_qkv.shape, BF16),
            pltpu.VMEM(x.shape, BF16), pltpu.VMEM(w_t.shape[1:], BF16),
            pltpu.VMEM(k_t.shape[1:], BF16), pltpu.VMEM(v_t.shape[1:], BF16),
            pltpu.VMEM((nb, 128), BF16), pltpu.VMEM((nb // 128, 256, 128), BF16), pltpu.VMEM((nb, 128), BF16),
            pltpu.SemaphoreType.DMA((2, groups)), pltpu.SemaphoreType.DMA((2, groups)), pltpu.SemaphoreType.DMA((groups,)), pltpu.SemaphoreType.DMA((6,))],
        input_output_aliases=aliases,
        compiler_params=pltpu.CompilerParams(vmem_limit_bytes=ATTN_VMEM),
        cost_estimate=pl.CostEstimate(flops=10 ** 9, bytes_accessed=2 ** 25, transcendentals=0),
        name=f"attention_{layer}",
    )(*operands)


PIECES = 2


def tail_kernel(layer, last, a_hbm, x_hbm, gain_hbm, bias_hbm, bo_hbm, bu_hbm, bd_hbm, wo_hbm, wu_hbm, wd_hbm, *rest):
    if last:
        out_hbm, *rest = rest
    else:
        out_hbm, xrow_out, *rest = rest
    (a_s, gain_ref, bias_ref, bo_ref, bu, bd_ref, wo, wu, wd, xs, bu_x, wu_x, wd_x, hb, ob, own, dsend, drecv, csend, crecv,
     w_sem, o_sem, xs_sem, xr_sem, ds_sem, dr_sem, cs_sem, cr_sem, hs_sem, hr_sem, gs_sem, gr_sem) = rest
    nb = ob.shape[0]
    me = lax.axis_index("tp")
    core = lax.rem(me, 2)
    chip = lax.div(me, 2)
    half = nb // 2
    cut = nb // 8
    piece = cut // PIECES
    pieces = range(PIECES)
    far = (3, 1, 2)

    def chip_at(dist):
        xb, yb = lax.rem(chip, 2), lax.div(chip, 2)
        dx, dy = dist % 2, dist // 2
        return (yb + dy - 2 * dy * yb) * 2 + xb + dx - 2 * dx * xb

    sibling = chip * 2 + 1 - core
    peers = {d: chip_at(d) * 2 + core for d in far}

    def send(src, dst, s_sem, r_sem, dev):
        return pltpu.make_async_remote_copy(src, dst, s_sem, r_sem, device_id={"tp": dev}, device_id_type=MESH)

    def slot(d, s):
        return pl.ds(pl.multiple_of(chip_at(d) * cut + s * piece, piece), piece)

    def at(s):
        return pl.ds(s * piece, piece)

    row0 = pl.multiple_of(core * half + chip * cut, cut)
    x_mine = x_hbm.at[pl.ds(row0, cut)] if layer == 0 else x_hbm
    pairs = [(a_hbm, a_s), (wo_hbm.at[layer], wo), (x_mine, xs), (gain_hbm, gain_ref), (bias_hbm, bias_ref), (bo_hbm, bo_ref),
             (bu_hbm, bu), (bd_hbm, bd_ref), (wu_hbm.at[layer], wu), (wd_hbm.at[layer], wd)]
    loads = [pltpu.make_async_copy(src, dst, w_sem.at[i]) for i, (src, dst) in enumerate(pairs)]
    for cp in loads:
        cp.start()
    barrier = pltpu.get_barrier_semaphore()
    for dev in [sibling] + [peers[d] for d in far]:
        pl.semaphore_signal(barrier, inc=1, device_id={"tp": dev}, device_id_type=MESH)

    for cp in loads[:2]:
        cp.wait()
    dsend[...] = jnp.dot(a_s[pl.ds(pl.multiple_of((1 - core) * half, half), half), :], wo[...], preferred_element_type=F32).astype(BF16)
    pl.semaphore_wait(barrier, 4)
    d2d = {(s, d): send(dsend.at[slot(d, s)], drecv.at[slot(d, s)], ds_sem.at[s, n], dr_sem.at[s, n], sibling)
           for s in pieces for n, d in enumerate(far + (0,))}
    for cp in d2d.values():
        cp.start()
    swap = [send(src, dst, xs_sem.at[n], xr_sem.at[n], sibling)
            for n, (src, dst) in enumerate(((bu_hbm, bu_x), (wu_hbm.at[layer], wu_x), (wd_hbm.at[layer], wd_x)))]
    for cp in swap:
        cp.start()
    own[...] = jnp.dot(a_s[pl.ds(pl.multiple_of(core * half, half), half), :], wo[...], preferred_element_type=F32)
    sends = {}

    def reduce_to(r, s, d, part):
        n = far.index(d)
        csend[r, n, at(s), :] = part.astype(BF16)
        sends[r, s, d] = send(csend.at[r, n, at(s)], crecv.at[r, n, at(s)], cs_sem.at[r, s, n], cr_sem.at[r, s, n], peers[d])
        sends[r, s, d].start()

    def received(r, s, total):
        for d in (2, 3, 1):
            sends[r, s, d].wait_recv()
            total = total + crecv[r, far.index(d), at(s), :].astype(F32)
        return total

    for s in pieces:
        for d in far:
            d2d[s, d].wait_recv()
            reduce_to(0, s, d, own[slot(d, s), :] + drecv[slot(d, s), :].astype(F32))
    for cp in loads[2:]:
        cp.wait()
    xmid, hsend = {}, {}
    for s in pieces:
        d2d[s, 0].wait_recv()
        total = received(0, s, own[slot(0, s), :] + drecv[slot(0, s), :].astype(F32))
        xmid[s] = (xs[at(s), :].astype(F32) + total + bo_ref[...].astype(F32)[layer:layer + 1]).astype(BF16)
        mine = hb.at[slot(0, s)]
        mine[...] = norm_rows(xmid[s].astype(F32), gain_ref[layer, 1:2, :], bias_ref[layer, 1:2, :])
        for n, d in enumerate(far):
            hsend[s, d] = send(mine, mine, hs_sem.at[s, n], hr_sem.at[s, n], peers[d])
            hsend[s, d].start()

    for cp in swap:
        cp.wait_recv()

    def mlp(h):
        part = None
        for b_ref, u_ref, w_ref in ((bu, wu, wd), (bu_x, wu_x, wd_x)):
            up = jnp.dot(h, u_ref[...], preferred_element_type=F32) + b_ref[...].astype(F32)[layer:layer + 1]
            y = jnp.dot(jnp.maximum(up, 0.0).astype(BF16), w_ref[...], preferred_element_type=F32)
            part = y if part is None else part + y
        return part

    own[0:cut, :] = mlp(jnp.concatenate([hb[slot(0, s), :] for s in pieces], axis=0))
    for s in pieces:
        for n, d in enumerate(far):
            send(hb.at[slot(0, s)], hb.at[slot(d, s)], hs_sem.at[s, n], hr_sem.at[s, n], peers[d]).wait_recv()
        part = mlp(jnp.concatenate([hb[slot(d, s), :] for d in far], axis=0))
        for n, d in enumerate(far):
            reduce_to(1, s, d, part[n * piece:(n + 1) * piece])

    def place(d, k, s):
        return pl.ds(pl.multiple_of(k * half + chip_at(d) * cut + s * piece, piece), piece)

    kept = []

    def keep(d, k, s, n):
        kept.append(pltpu.make_async_copy(ob.at[place(d, k, s)], out_hbm.at[place(d, k, s)], o_sem.at[s, n]))
        kept[-1].start()

    spread = {}
    for s in pieces:
        total = received(1, s, own[at(s), :])
        xnew = (xmid[s].astype(F32) + total + bd_ref[...].astype(F32)[layer:layer + 1]).astype(BF16)
        mine = ob.at[place(0, core, s)]
        if last:
            mine[...] = xnew
        else:
            mine[...] = norm_rows(xnew.astype(F32), gain_ref[layer + 1, 0:1, :], bias_ref[layer + 1, 0:1, :])
        for n, (d, dev) in enumerate([(d, peers[d]) for d in far] + [(0, sibling)]):
            spread[s, d] = send(mine, mine, gs_sem.at[s, n], gr_sem.at[s, n], dev)
            spread[s, d].start()
        keep(0, core, s, 0)
        if not last:
            xs[at(s), :] = xnew
            kept.append(pltpu.make_async_copy(xs.at[at(s)], xrow_out.at[at(s)], o_sem.at[s, 8]))
            kept[-1].start()
    passed = {}
    for s in pieces:
        for d in (2, 3, 1):
            n = far.index(d)
            block = ob.at[place(d, core, s)]
            send(ob.at[place(0, core, s)], block, gs_sem.at[s, n], gr_sem.at[s, n], peers[d]).wait_recv()
            passed[s, d] = send(block, block, gs_sem.at[s, 4 + n], gr_sem.at[s, 4 + n], sibling)
            passed[s, d].start()
            keep(d, core, s, 1 + n)
    for s in pieces:
        spread[s, 0].wait_recv()
        keep(0, 1 - core, s, 4)
        for d in (2, 3, 1):
            passed[s, d].wait_recv()
            keep(d, 1 - core, s, 5 + far.index(d))
    for cp in [*d2d.values(), *swap, *sends.values(), *hsend.values(), *spread.values(), *passed.values()]:
        cp.wait_send()
    for cp in kept:
        cp.wait()


def tail(layer, last, a, x, gain, bias, b_out, b_up, b_down, w_out, w_up, w_down):
    nb = a.shape[0]
    width = w_out.shape[-1]
    half, cut = nb // 2, nb // 8
    hbm = pl.BlockSpec(memory_space=pltpu.HBM)
    out_shape = [jax.ShapeDtypeStruct((nb, width), BF16)]
    if not last:
        out_shape.append(jax.ShapeDtypeStruct((cut, width), BF16))
    dma = pltpu.SemaphoreType.DMA
    return pl.pallas_call(
        functools.partial(tail_kernel, layer, last),
        in_specs=[hbm] * 10,
        out_specs=[hbm] * len(out_shape),
        out_shape=out_shape,
        scratch_shapes=[
            pltpu.VMEM(a.shape, BF16), pltpu.VMEM(gain.shape, F32), pltpu.VMEM(bias.shape, F32),
            pltpu.VMEM(b_out.shape, BF16), pltpu.VMEM(b_up.shape, BF16), pltpu.VMEM(b_down.shape, BF16),
            pltpu.VMEM(w_out.shape[1:], BF16), pltpu.VMEM(w_up.shape[1:], BF16), pltpu.VMEM(w_down.shape[1:], BF16),
            pltpu.VMEM((cut, width), BF16),
            pltpu.VMEM(b_up.shape, BF16), pltpu.VMEM(w_up.shape[1:], BF16), pltpu.VMEM(w_down.shape[1:], BF16),
            pltpu.VMEM((half, width), BF16), pltpu.VMEM((nb, width), BF16), pltpu.VMEM((half, width), F32),
            pltpu.VMEM((half, width), BF16), pltpu.VMEM((half, width), BF16),
            pltpu.VMEM((2, 3, cut, width), BF16), pltpu.VMEM((2, 3, cut, width), BF16),
            dma((10,)), dma((PIECES, 9)), dma((3,)), dma((3,)), dma((PIECES, 4)), dma((PIECES, 4)),
            dma((2, PIECES, 3)), dma((2, PIECES, 3)), dma((PIECES, 3)), dma((PIECES, 3)), dma((PIECES, 7)), dma((PIECES, 7))],
        compiler_params=pltpu.CompilerParams(collective_id=layer, has_side_effects=True, vmem_limit_bytes=ATTN_VMEM),
        cost_estimate=pl.CostEstimate(flops=10 ** 9, bytes_accessed=2 ** 22, transcendentals=0),
        name=f"tail_{layer}",
    )(a, x, gain, bias, b_out, b_up, b_down, w_out, w_up, w_down)


def solution(mesh):
    cache_spec = P(None, 'dp', 'tp', None, None)
    in_specs = (P('dp', None), P('dp'), cache_spec, cache_spec, P(), P(),
                P(None, None, None, 'tp', None), P(None, None, 'tp', None),
                P(None, 'tp', None, None), P(), P(None, None, 'tp'), P(None, 'tp'),
                P(None, 'tp', None), P())
    out_specs = (P('dp', None), cache_spec, cache_spec)

    def local_step(x, cache_len, k_cache, v_cache, norm_gain, norm_bias, w_qkv, b_qkv, w_out, b_out, w_up, b_up, w_down, b_down):
        layers = k_cache.shape[0]
        width = x.shape[1]
        k_t, v_t = k_cache.swapaxes(3, 4), v_cache.swapaxes(3, 4)
        w_t = w_qkv.transpose(0, 2, 3, 4, 1).reshape(layers, -1, width)
        w_o = w_out.reshape(layers, -1, width)
        h, xrow, caches = x, x, None
        for layer in range(layers):
            last = layer == layers - 1
            *caches, att = attention(layer, cache_len, h, norm_gain, norm_bias, w_t, b_qkv, k_t, v_t, caches)
            outs = tail(layer, last, att, xrow, norm_gain, norm_bias, b_out, b_up, b_down, w_o, w_up, w_down)
            h = outs[0]
            if not last:
                xrow = outs[1]
        return h, caches[0].swapaxes(3, 4), caches[1].swapaxes(3, 4)

    return jax.shard_map(local_step, mesh=mesh, in_specs=in_specs, out_specs=out_specs, check_vma=False)
```
